32 devices in a mesh: cls: 32 (over z, y, x, core).
Axes of the slice: x: 2, y: 2, z: 4, core: 2. Of those that a mesh axis runs over, the one named last changes fastest.
Arguments:
- features: bfloat16 [512, 12544], P('cls'), may hold values from -6 to 6
- fc_weight: bfloat16 [12544, 512], replicated, may hold values from -0.0546875 to 0.0546875
- centers: bfloat16 [131072, 512], P('cls'), may hold values from -6 to 6
- labels: int32 [512], replicated, may hold values from 0 to 131071
Outputs:
- loss: float32 [512], P('cls')
- grad_centers: bfloat16 [131072, 512], P('cls')
- grad_fc: float32 [12544, 512], P('cls')
The draws below stay inside these ranges and needn't reach their ends.
All inputs are finite; a program needn't handle non-finite values.
Results may differ from the reference program's by a relative error of at most 0.0078.
Values may be sent and summed in bfloat16 or wider, within the bound.
A program may use at most 128 MiB of HBM per device.

```python
import math
import jax
import jax.numpy as jnp
from jax import lax

D = 512
F = 12544
C_DEV = 4096
B = 512
C = 131072
N_CLS = 32


def place_ends(entries, own_key, least, top_value):
    longest = entries.shape.index(max(entries.shape))
    spots = []
    for shift in (0, 1):
        where = [jax.random.randint(jax.random.fold_in(own_key, axis), (), 0, length) for axis, length in enumerate(entries.shape)]
        where[longest] = (where[longest] + shift) % entries.shape[longest]
        spots.append(tuple(where))
    return entries.at[spots[0]].set(least).at[spots[1]].set(top_value)


def levels(key, shape, cuts, smallest, largest):
    level, own = 1.0, jax.random.fold_in(key, 6)
    for position, blocks in cuts:
        steps = jnp.exp(jax.random.uniform(jax.random.fold_in(own, position), (blocks,), jnp.float32, smallest / len(cuts), largest / len(cuts)))
        level = level * jnp.repeat(steps, shape[position] // blocks).reshape([-1 if axis == position else 1 for axis in range(len(shape))])
    return level


def gaussian(key, shape, deviation, reach, split=(), held_as=jnp.bfloat16):
    result = deviation * jax.random.normal(key, shape, jnp.float32)
    if split:
        result = result * levels(key, shape, split, -0.22, 0.18)
    return jnp.clip(result, -reach, reach).astype(held_as)


def setup_inputs(seed: int = 0) -> dict:
    key_list = jax.random.split(jax.random.key(seed), 5)
    return {
        "features": gaussian(key_list[0], (B, F), 1.0, 6.0, ((0, 32),)),
        "fc_weight": gaussian(key_list[1], (F, D), F ** -0.5, 0.0546875),
        "centers": gaussian(key_list[2], (C, D), 1.0, 6.0, ((0, 32),)),
        "labels": place_ends(jax.random.randint(key_list[3], (B,), 0, C), jax.random.fold_in(key_list[3], 1), 0, C - 1).astype(jnp.int32),
    }


logit_scale = 64.0
cos_margin = math.cos(0.5)
sin_margin = math.sin(0.5)
epsilon = 1e-06

def inverse_norm(values):
    return lax.rsqrt(lax.optimization_barrier(jnp.sum(values * values, axis=1, keepdims=True)) + epsilon)

def margin_logits(emb_low, center_low, labels, offset):
    cosines = jnp.dot(emb_low, center_low.T, preferred_element_type=jnp.float32)
    local_ids = labels - offset
    is_target = local_ids[:, None] == lax.broadcasted_iota(jnp.int32, (1, center_low.shape[0]), 1)
    target_cos = lax.optimization_barrier(jnp.sum(jnp.where(is_target, cosines, 0.0), axis=1))
    target_sine = jnp.sqrt(1.0 - target_cos * target_cos)
    margined = target_cos * cos_margin - target_sine * sin_margin
    logits = logit_scale * jnp.where(is_target, margined[:, None], cosines)
    slope = cos_margin + sin_margin * target_cos / target_sine
    return (logits, is_target, slope)

def center_parts(block):
    center_float = block.astype(jnp.float32)
    inv_center = inverse_norm(center_float)
    center_dir = center_float * inv_center
    return (inv_center, center_dir, center_dir.astype(jnp.bfloat16))

def reference(features, fc_weight, centers, labels):
    batch = labels.shape[0]
    embedded = jnp.dot(features, fc_weight, preferred_element_type=jnp.float32).astype(jnp.bfloat16)
    emb_float = embedded.astype(jnp.float32)
    inv_emb = inverse_norm(emb_float)
    emb_dir = emb_float * inv_emb
    emb_low = emb_dir.astype(jnp.bfloat16)
    blocks = centers.reshape(N_CLS, C_DEV, D)
    shard_ids = jnp.arange(N_CLS, dtype=jnp.int32)

    def stats_step(carry, item):
        shard, block = item
        unused_inv, unused_dir, center_low = center_parts(block)
        logits, is_target, unused_slope = margin_logits(emb_low, center_low, labels, shard * C_DEV)
        running_sum, target_sum = carry
        running_sum = running_sum + lax.optimization_barrier(jnp.sum(jnp.exp(logits - logit_scale), axis=1))
        target_sum = target_sum + lax.optimization_barrier(jnp.sum(jnp.where(is_target, logits, 0.0), axis=1))
        return ((running_sum, target_sum), None)
    start_stats = (jnp.zeros((batch,), jnp.float32), jnp.zeros((batch,), jnp.float32))
    (row_sum, target_sum), unused_out = lax.scan(stats_step, start_stats, (shard_ids, blocks))
    log_total = logit_scale + jnp.log(row_sum)
    loss = log_total - target_sum

    def grad_step(grad_dir, item):
        shard, block = item
        inv_center, center_dir, center_low = center_parts(block)
        logits, is_target, slope = margin_logits(emb_low, center_low, labels, shard * C_DEV)
        probs = jnp.exp(logits - log_total[:, None])
        grad_cos = (logit_scale * (probs - is_target.astype(jnp.float32)) * jnp.where(is_target, slope[:, None], 1.0)).astype(jnp.bfloat16)
        grad_unit = jnp.dot(grad_cos.T, emb_low, preferred_element_type=jnp.float32)
        grad_center = ((grad_unit - center_dir * lax.optimization_barrier(jnp.sum(grad_unit * center_dir, axis=1, keepdims=True))) * inv_center).astype(jnp.bfloat16)
        grad_dir = grad_dir + jnp.dot(grad_cos, center_low, preferred_element_type=jnp.float32)
        return (grad_dir, grad_center)
    grad_dir, grad_blocks = lax.scan(grad_step, jnp.zeros((batch, D), jnp.float32), (shard_ids, blocks))
    grad_centers = grad_blocks.reshape(N_CLS * C_DEV, D)
    grad_emb = ((grad_dir - emb_dir * lax.optimization_barrier(jnp.sum(grad_dir * emb_dir, axis=1, keepdims=True))) * inv_emb).astype(jnp.bfloat16)
    grad_fc = jnp.dot(features.T, grad_emb, preferred_element_type=jnp.float32)
    return (loss, grad_centers, grad_fc)
```

```python
import math

import jax
import jax.numpy as jnp
from jax import lax
from jax.sharding import PartitionSpec as P

logit_scale = 64.0
cos_margin = math.cos(0.5)
sin_margin = math.sin(0.5)
epsilon = 1e-06


def inverse_norm(values):
    return lax.rsqrt(jnp.sum(values * values, axis=1, keepdims=True) + epsilon)


def margin_logits(emb_low, center_low, labels, offset):
    cosines = lax.dot_general(
        emb_low, center_low, (((1,), (1,)), ((), ())), preferred_element_type=jnp.float32
    )
    local_ids = labels - offset
    is_target = local_ids[:, None] == lax.broadcasted_iota(jnp.int32, (1, center_low.shape[0]), 1)
    target_cos = jnp.sum(jnp.where(is_target, cosines, 0.0), axis=1)
    target_sine = jnp.sqrt(1.0 - target_cos * target_cos)
    margined = target_cos * cos_margin - target_sine * sin_margin
    logits = logit_scale * jnp.where(is_target, margined[:, None], cosines)
    slope = cos_margin + sin_margin * target_cos / target_sine
    return (logits, is_target, slope)


def swap(blocks):
    return lax.all_to_all(blocks, "cls", split_axis=0, concat_axis=0, tiled=True)


def spread(block, count):
    return swap(jnp.broadcast_to(block[None], (count, *block.shape)))


def on_device(features, fc_weight, centers, labels):
    tok_rows = features.shape[0]
    class_rows = centers.shape[0]
    my_index = lax.axis_index("cls")
    count = lax.axis_size("cls")
    columns = lax.all_to_all(features, "cls", split_axis=1, concat_axis=0, tiled=True)
    embedded = jnp.dot(features, fc_weight, preferred_element_type=jnp.float32).astype(jnp.bfloat16)
    gathered = spread(embedded, count).reshape(count * tok_rows, -1)
    all_float = gathered.astype(jnp.float32)
    emb_low = (all_float * inverse_norm(all_float)).astype(jnp.bfloat16)
    own_float = embedded.astype(jnp.float32)
    inv_emb = inverse_norm(own_float)
    emb_dir = own_float * inv_emb
    center_float = centers.astype(jnp.float32)
    inv_center = inverse_norm(center_float)
    center_dir = center_float * inv_center
    center_low = center_dir.astype(jnp.bfloat16)
    logits, is_target, slope = margin_logits(emb_low, center_low, labels, my_index * class_rows)
    target_logit = jnp.sum(jnp.where(is_target, logits, 0.0), axis=1)
    stats = jnp.stack([jnp.sum(jnp.exp(logits - logit_scale), axis=1), target_logit])
    row_total, target_all = jnp.sum(spread(stats, count), axis=0)
    log_total = logit_scale + jnp.log(row_total)
    loss = lax.dynamic_slice_in_dim(log_total - target_all, my_index * tok_rows, tok_rows)
    probs = jnp.exp(logits - log_total[:, None])
    grad_cos = (
        logit_scale
        * (probs - is_target.astype(jnp.float32))
        * jnp.where(is_target, slope[:, None], 1.0)
    ).astype(jnp.bfloat16)
    grad_unit = lax.dot_general(
        grad_cos, emb_low, (((0,), (0,)), ((), ())), preferred_element_type=jnp.float32
    )
    grad_centers = (
        (grad_unit - center_dir * jnp.sum(grad_unit * center_dir, axis=1, keepdims=True))
        * inv_center
    ).astype(jnp.bfloat16)
    partial = jnp.dot(grad_cos, center_low, preferred_element_type=jnp.float32)
    parts = swap(partial.astype(jnp.bfloat16).reshape(count, tok_rows, -1))
    grad_dir = jnp.sum(parts.astype(jnp.float32), axis=0)
    grad_emb = (
        (grad_dir - emb_dir * jnp.sum(grad_dir * emb_dir, axis=1, keepdims=True)) * inv_emb
    ).astype(jnp.bfloat16)
    all_grads = spread(grad_emb, count).reshape(count * tok_rows, -1)
    grad_fc = lax.dot_general(
        columns, all_grads, (((0,), (0,)), ((), ())), preferred_element_type=jnp.float32
    )
    return (loss, grad_centers, grad_fc)


def solution(mesh):
    placed = (P("cls", None), P(), P("cls", None), P())
    return jax.shard_map(
        on_device,
        mesh=mesh,
        in_specs=placed,
        out_specs=(P("cls"), P("cls", None), P("cls", None)),
        check_vma=False,
    )
```

```python
import functools
import math

import jax
import jax.numpy as jnp
from jax import lax
from jax.experimental import pallas as pl
from jax.experimental.pallas import tpu as pltpu
from jax.sharding import PartitionSpec as P

logit_scale = 64.0
cos_margin = math.cos(0.5)
sin_margin = math.sin(0.5)
epsilon = 1e-06
MESH = pl.DeviceIdType.MESH
f32, bf16 = jnp.float32, jnp.bfloat16


def inverse_norm(values):
    return lax.rsqrt(jnp.sum(values * values, axis=1, keepdims=True) + epsilon)


def largest_divisor(number, most):
    return next(d for d in range(most, 0, -1) if number % d == 0)


def kernel(
    n, rows, slots, feat, weight, centers_hbm, labels,
    loss_out, gc_out, cols_out, grads_out,
    wbuf, cbuf, clow, inv_c, cosines, acc, esend, emb, fsend, frecv,
    ssend, srecv, psend, precv, gsend, grecv, stage,
    wsem, csem, osem, ksem, ssems, rsems,
):
    me = lax.axis_index("cls")
    tok, feats = feat.shape
    classes, width = cbuf.shape
    batch = n * tok
    chunk = wbuf.shape[1]
    chunks = feats // chunk
    blocks = classes // rows
    part = feats // n
    half = n // 2

    def weight_copy(c):
        return pltpu.make_async_copy(
            weight.at[pl.ds(c * chunk, chunk)], wbuf.at[c % slots], wsem.at[c % slots]
        )

    for c in range(min(slots, chunks)):
        weight_copy(c).start()
    centers_copy = pltpu.make_async_copy(centers_hbm, cbuf, csem)
    centers_copy.start()

    barrier = pltpu.get_barrier_semaphore()

    def greet(i, carry):
        pl.semaphore_signal(barrier, inc=1, device_id=(lax.rem(me + i, n),), device_id_type=MESH)
        return carry

    lax.fori_loop(1, n, greet, 0)

    for j in range(n):
        fsend[j] = feat[:, j * part : (j + 1) * part]

    total = jnp.zeros((tok, width), f32)
    for c in range(chunks):
        weight_copy(c).wait()
        total = total + jnp.dot(
            feat[:, c * chunk : (c + 1) * chunk], wbuf[c % slots], preferred_element_type=f32
        )
        if c + slots < chunks:
            weight_copy(c + slots).start()
    esend[...] = total.astype(bf16)
    emb[me] = total.astype(bf16)
    pl.semaphore_wait(barrier, n - 1)

    def send_to(phase, source, target, first, last):
        def step(i, carry):
            dst = lax.rem(me + i, n)
            pltpu.make_async_remote_copy(
                src_ref=source(dst), dst_ref=target.at[me],
                send_sem=ssems.at[phase], recv_sem=rsems.at[phase],
                device_id=(dst,), device_id_type=MESH,
            ).start()
            return carry

        lax.fori_loop(first, last, step, 0)

    def wait_all(sems, phase, target):
        whole = target.at[pl.ds(0, n - 1)]
        pltpu.make_async_copy(whole, whole, sems.at[phase]).wait()

    send_to(0, lambda dst: esend, emb, 1, n)

    centers_copy.wait()

    def normalise(k, carry):
        at = pl.ds(pl.multiple_of(k * rows, rows), rows)
        block = cbuf[at].astype(f32)
        inv = inverse_norm(block)
        inv_c[at] = inv
        clow[at] = (block * inv).astype(bf16)
        return carry

    lax.fori_loop(0, blocks, normalise, 0)

    wait_all(rsems, 0, emb)
    send_to(1, lambda dst: fsend.at[dst], frecv, 1, half)
    frecv[me] = fsend[me]

    all_emb = emb[...].reshape(batch, width).astype(f32)
    emb_low = (all_emb * inverse_norm(all_emb)).astype(bf16)
    emb[...] = emb_low.reshape(n, tok, width)

    local = labels[...] - me * classes
    class_ids = lax.broadcasted_iota(jnp.int32, (rows, batch), 0)

    def forward(k, carry):
        esum, tcos = carry
        at = pl.ds(pl.multiple_of(k * rows, rows), rows)
        cos = lax.dot_general(
            clow[at], emb[...].reshape(batch, width), (((1,), (1,)), ((), ())),
            preferred_element_type=f32,
        )
        cosines[at] = cos
        hit = class_ids == local - k * rows
        tcos = tcos + jnp.sum(jnp.where(hit, cos, 0.0), axis=0, keepdims=True)
        powers = jnp.exp(logit_scale * cos - logit_scale)
        esum = esum + jnp.sum(jnp.where(hit, 0.0, powers), axis=0, keepdims=True)
        return esum, tcos

    zero_row = jnp.zeros((1, batch), f32)
    esum, tcos = lax.fori_loop(0, blocks, forward, (zero_row, zero_row))
    mine = (local >= 0) & (local < classes)
    tsin = jnp.sqrt(1.0 - tcos * tcos)
    tlogit = logit_scale * (tcos * cos_margin - tsin * sin_margin)
    slope = cos_margin + sin_margin * tcos / tsin
    esum = esum + jnp.where(mine, jnp.exp(tlogit - logit_scale), 0.0)
    ssend[0:1] = esum
    ssend[1:2] = jnp.where(mine, tlogit, 0.0)
    srecv[me] = ssend[...]
    send_to(2, lambda dst: ssend, srecv, 1, n)
    wait_all(rsems, 2, srecv)
    send_to(1, lambda dst: fsend.at[dst], frecv, half, n)
    stats = jnp.sum(srecv[...], axis=0)
    log_total = logit_scale + jnp.log(stats[0:1])
    loss_out[...] = log_total - stats[1:2]
    tgrad = logit_scale * (jnp.exp(tlogit - log_total) - 1.0) * slope

    def grad_cos(k):
        at = pl.ds(pl.multiple_of(k * rows, rows), rows)
        hit = class_ids == local - k * rows
        probs = jnp.exp(logit_scale * cosines[at] - log_total)
        return jnp.where(hit, tgrad, logit_scale * probs).astype(bf16)

    acc[...] = jnp.zeros_like(acc)

    def embed_grads(k, carry):
        at = pl.ds(pl.multiple_of(k * rows, rows), rows)
        acc[...] += lax.dot_general(
            grad_cos(k), clow[at], (((0,), (0,)), ((), ())), preferred_element_type=f32
        )
        return carry

    lax.fori_loop(0, blocks, embed_grads, 0)
    psend[...] = acc[...].astype(bf16).reshape(n, tok, width)
    precv[me] = psend[me]
    send_to(3, lambda dst: psend.at[dst], precv, 1, n)

    def out_copy(k, slot):
        at = pl.ds(pl.multiple_of(k * rows, rows), rows)
        return pltpu.make_async_copy(stage.at[slot], gc_out.at[at], osem.at[slot])

    def center_grads(k, carry):
        at = pl.ds(pl.multiple_of(k * rows, rows), rows)
        unit = jnp.dot(
            grad_cos(k), emb[...].reshape(batch, width), preferred_element_type=f32
        )
        inv = inv_c[at]
        direction = cbuf[at].astype(f32) * inv
        along = jnp.sum(unit * direction, axis=1, keepdims=True)
        slot = lax.rem(k, 2)

        @pl.when(k >= 2)
        def _():
            out_copy(k - 2, slot).wait()

        stage[slot] = ((unit - direction * along) * inv).astype(bf16)
        out_copy(k, slot).start()
        return carry

    lax.fori_loop(0, blocks, center_grads, 0)

    wait_all(rsems, 3, precv)
    grad_dir = jnp.sum(precv[...].astype(f32), axis=0)
    own = esend[...].astype(f32)
    inv_emb = inverse_norm(own)
    emb_dir = own * inv_emb
    along = jnp.sum(grad_dir * emb_dir, axis=1, keepdims=True)
    grad_emb = ((grad_dir - emb_dir * along) * inv_emb).astype(bf16)
    gsend[...] = grad_emb
    grecv[me] = grad_emb
    send_to(4, lambda dst: gsend, grecv, 1, n)

    wait_all(rsems, 1, frecv)
    cols_copy = pltpu.make_async_copy(frecv, cols_out, ksem.at[0])
    cols_copy.start()
    for k in range(max(blocks - 2, 0), blocks):
        out_copy(k, k % 2).wait()
    wait_all(rsems, 4, grecv)
    grads_copy = pltpu.make_async_copy(grecv, grads_out, ksem.at[1])
    grads_copy.start()
    for phase, target in ((0, emb), (1, frecv), (2, srecv), (3, precv), (4, grecv)):
        wait_all(ssems, phase, target)
    cols_copy.wait()
    grads_copy.wait()


def on_device(features, fc_weight, centers, labels):
    n = lax.axis_size("cls")
    tok, feats = features.shape
    classes, width = centers.shape
    batch = labels.shape[0]
    rows = min(512, 262144 // batch)
    slots = 4 if batch <= 1024 else 2
    chunk = feats // 128 // 7 * 128
    chunk = 128 * largest_divisor(feats // 128, 14)
    part = feats // n
    vmem = pl.BlockSpec(memory_space=pltpu.VMEM)
    hbm = pl.BlockSpec(memory_space=pl.ANY)
    loss_row, grad_centers, columns, all_grads = pl.pallas_call(
        functools.partial(kernel, n, rows, slots),
        out_shape=(
            jax.ShapeDtypeStruct((1, batch), f32),
            jax.ShapeDtypeStruct((classes, width), bf16),
            jax.ShapeDtypeStruct((n, tok, part), bf16),
            jax.ShapeDtypeStruct((n, tok, width), bf16),
        ),
        in_specs=[vmem, hbm, hbm, vmem],
        out_specs=(vmem, hbm, hbm, hbm),
        scratch_shapes=[
            pltpu.VMEM((slots, chunk, width), bf16),
            pltpu.VMEM((classes, width), bf16),
            pltpu.VMEM((classes, width), bf16),
            pltpu.VMEM((classes, 1), f32),
            pltpu.VMEM((classes, batch), f32),
            pltpu.VMEM((batch, width), f32),
            pltpu.VMEM((tok, width), bf16),
            pltpu.VMEM((n, tok, width), bf16),
            pltpu.VMEM((n, tok, part), bf16),
            pltpu.VMEM((n, tok, part), bf16),
            pltpu.VMEM((2, batch), f32),
            pltpu.VMEM((n, 2, batch), f32),
            pltpu.VMEM((n, tok, width), bf16),
            pltpu.VMEM((n, tok, width), bf16),
            pltpu.VMEM((tok, width), bf16),
            pltpu.VMEM((n, tok, width), bf16),
            pltpu.VMEM((2, rows, width), bf16),
            pltpu.SemaphoreType.DMA((slots,)),
            pltpu.SemaphoreType.DMA,
            pltpu.SemaphoreType.DMA((2,)),
            pltpu.SemaphoreType.DMA((2,)),
            pltpu.SemaphoreType.DMA((5,)),
            pltpu.SemaphoreType.DMA((5,)),
        ],
        compiler_params=pltpu.CompilerParams(
            collective_id=0, has_side_effects=True, vmem_limit_bytes=67043328
        ),
    )(features, fc_weight, centers, labels[None])
    loss = lax.dynamic_slice_in_dim(loss_row[0], lax.axis_index("cls") * tok, tok)
    grad_fc = lax.dot_general(
        columns.reshape(batch, part), all_grads.reshape(batch, width),
        (((0,), (0,)), ((), ())), preferred_element_type=f32,
    )
    return (loss, grad_centers, grad_fc)


def solution(mesh):
    placed = (P("cls", None), P(), P("cls", None), P())
    return jax.shard_map(
        on_device,
        mesh=mesh,
        in_specs=placed,
        out_specs=(P("cls"), P("cls", None), P("cls", None)),
        check_vma=False,
    )
```

```python
import functools
import math

import jax
import jax.numpy as jnp
from jax import lax
from jax.experimental import pallas as pl
from jax.experimental.pallas import tpu as pltpu
from jax.sharding import PartitionSpec as P

logit_scale = 64.0
cos_margin = math.cos(0.5)
sin_margin = math.sin(0.5)
epsilon = 1e-06
MESH = pl.DeviceIdType.MESH
f32, bf16 = jnp.float32, jnp.bfloat16


def inverse_norm(values):
    return lax.rsqrt(jnp.sum(values * values, axis=1, keepdims=True) + epsilon)


def largest_divisor(number, most):
    return next(d for d in range(most, 0, -1) if number % d == 0)


def kernel(
    n, rows, slots, feat, weight, centers_hbm, labels,
    loss_out, gc_out, fc_out,
    wbuf, cbuf, clow, inv_c, cosines, acc, esend, emb, fsend, frecv,
    ssend, srecv, psend, pair, precv, gsend, grecv, stage,
    wsem, csem, osem, ssems, rsems,
):
    me = lax.axis_index("cls")
    tok, feats = feat.shape
    classes, width = cbuf.shape
    batch = n * tok
    chunk = wbuf.shape[1]
    chunks = feats // chunk
    blocks = classes // rows
    part = feats // n
    half = n // 2
    core = lax.rem(me, 2)
    chip = me // 2
    partner = me + 1 - 2 * core

    def weight_copy(c):
        return pltpu.make_async_copy(
            weight.at[pl.ds(c * chunk, chunk)], wbuf.at[c % slots], wsem.at[c % slots]
        )

    for c in range(min(slots, chunks)):
        weight_copy(c).start()
    centers_copy = pltpu.make_async_copy(centers_hbm, cbuf, csem)
    centers_copy.start()

    barrier = pltpu.get_barrier_semaphore()

    def greet(i, carry):
        pl.semaphore_signal(barrier, inc=1, device_id=(lax.rem(me + i, n),), device_id_type=MESH)
        return carry

    lax.fori_loop(1, n, greet, 0)

    for j in range(n):
        fsend[j] = feat[:, j * part : (j + 1) * part]

    total = jnp.zeros((tok, width), f32)
    for c in range(chunks):
        weight_copy(c).wait()
        total = total + jnp.dot(
            feat[:, c * chunk : (c + 1) * chunk], wbuf[c % slots], preferred_element_type=f32
        )
        if c + slots < chunks:
            weight_copy(c + slots).start()
    esend[...] = total.astype(bf16)
    emb[me] = total.astype(bf16)
    pl.semaphore_wait(barrier, n - 1)

    def send_to(phase, source, target, first, last):
        def step(i, carry):
            dst = lax.rem(me + i, n)
            pltpu.make_async_remote_copy(
                src_ref=source(dst), dst_ref=target.at[me],
                send_sem=ssems.at[phase], recv_sem=rsems.at[phase],
                device_id=(dst,), device_id_type=MESH,
            ).start()
            return carry

        lax.fori_loop(first, last, step, 0)

    def wait_all(sems, phase, target, count):
        whole = target.at[pl.ds(0, count)]
        pltpu.make_async_copy(whole, whole, sems.at[phase]).wait()

    def send_chips(phase, source, target, slot):
        def step(i, carry):
            to = lax.rem(chip + i, half)
            pltpu.make_async_remote_copy(
                src_ref=source(to), dst_ref=target.at[slot],
                send_sem=ssems.at[phase], recv_sem=rsems.at[phase],
                device_id=(2 * to + core,), device_id_type=MESH,
            ).start()
            return carry

        lax.fori_loop(1, half, step, 0)

    def send_partner(phase, source, target):
        def step(j, carry):
            pltpu.make_async_remote_copy(
                src_ref=source(j), dst_ref=target(j),
                send_sem=ssems.at[phase], recv_sem=rsems.at[phase],
                device_id=(partner,), device_id_type=MESH,
            ).start()
            return carry

        lax.fori_loop(0, half, step, 0)

    send_chips(0, lambda to: esend, emb, me)

    centers_copy.wait()

    def normalise(k, carry):
        at = pl.ds(pl.multiple_of(k * rows, rows), rows)
        block = cbuf[at].astype(f32)
        inv = inverse_norm(block)
        inv_c[at] = inv
        clow[at] = (block * inv).astype(bf16)
        return carry

    lax.fori_loop(0, blocks, normalise, 0)

    wait_all(rsems, 0, emb, half - 1)
    send_partner(5, lambda j: emb.at[2 * j + core], lambda j: emb.at[2 * j + core])
    send_to(1, lambda dst: fsend.at[dst], frecv, 1, half)
    frecv[me] = fsend[me]
    wait_all(rsems, 5, emb, half)
    wait_all(ssems, 5, emb, half)

    all_emb = emb[...].reshape(batch, width).astype(f32)
    emb_low = (all_emb * inverse_norm(all_emb)).astype(bf16)
    emb[...] = emb_low.reshape(n, tok, width)

    local = labels[...] - me * classes
    class_ids = lax.broadcasted_iota(jnp.int32, (rows, batch), 0)

    def forward(k, carry):
        esum, tcos = carry
        at = pl.ds(pl.multiple_of(k * rows, rows), rows)
        cos = lax.dot_general(
            clow[at], emb[...].reshape(batch, width), (((1,), (1,)), ((), ())),
            preferred_element_type=f32,
        )
        cosines[at] = cos
        hit = class_ids == local - k * rows
        tcos = tcos + jnp.sum(jnp.where(hit, cos, 0.0), axis=0, keepdims=True)
        powers = jnp.exp(logit_scale * cos - logit_scale)
        esum = esum + jnp.sum(jnp.where(hit, 0.0, powers), axis=0, keepdims=True)
        return esum, tcos

    zero_row = jnp.zeros((1, batch), f32)
    esum, tcos = lax.fori_loop(0, blocks, forward, (zero_row, zero_row))
    mine = (local >= 0) & (local < classes)
    tsin = jnp.sqrt(1.0 - tcos * tcos)
    tlogit = logit_scale * (tcos * cos_margin - tsin * sin_margin)
    slope = cos_margin + sin_margin * tcos / tsin
    esum = esum + jnp.where(mine, jnp.exp(tlogit - logit_scale), 0.0)
    ssend[0:1] = esum
    ssend[1:2] = jnp.where(mine, tlogit, 0.0)
    srecv[me] = ssend[...]
    send_to(2, lambda dst: ssend, srecv, 1, n)
    wait_all(rsems, 2, srecv, n - 1)
    send_to(1, lambda dst: fsend.at[dst], frecv, half, n)
    stats = jnp.sum(srecv[...], axis=0)
    log_total = logit_scale + jnp.log(stats[0:1])
    loss_out[...] = log_total - stats[1:2]
    tgrad = logit_scale * (jnp.exp(tlogit - log_total) - 1.0) * slope

    def grad_cos(k):
        at = pl.ds(pl.multiple_of(k * rows, rows), rows)
        hit = class_ids == local - k * rows
        probs = jnp.exp(logit_scale * cosines[at] - log_total)
        return jnp.where(hit, tgrad, logit_scale * probs).astype(bf16)

    acc[...] = jnp.zeros_like(acc)

    def embed_grads(k, carry):
        at = pl.ds(pl.multiple_of(k * rows, rows), rows)
        acc[...] += lax.dot_general(
            grad_cos(k), clow[at], (((0,), (0,)), ((), ())), preferred_element_type=f32
        )
        return carry

    lax.fori_loop(0, blocks, embed_grads, 0)
    psend[...] = acc[...].astype(bf16).reshape(n, tok, width)
    send_partner(6, lambda j: psend.at[2 * j + 1 - core], lambda j: pair.at[j])

    def out_copy(k, slot):
        at = pl.ds(pl.multiple_of(k * rows, rows), rows)
        return pltpu.make_async_copy(stage.at[slot], gc_out.at[at], osem.at[slot])

    def center_grads(k, carry):
        at = pl.ds(pl.multiple_of(k * rows, rows), rows)
        unit = jnp.dot(
            grad_cos(k), emb[...].reshape(batch, width), preferred_element_type=f32
        )
        inv = inv_c[at]
        direction = cbuf[at].astype(f32) * inv
        along = jnp.sum(unit * direction, axis=1, keepdims=True)
        slot = lax.rem(k, 2)

        @pl.when(k >= 2)
        def _():
            out_copy(k - 2, slot).wait()

        stage[slot] = ((unit - direction * along) * inv).astype(bf16)
        out_copy(k, slot).start()
        return carry

    lax.fori_loop(0, 1, center_grads, 0)
    wait_all(rsems, 6, pair, half)

    def add_pair(j, carry):
        at = pl.ds(pl.multiple_of((2 * j + core) * tok, tok), tok)
        psend[2 * j + core] = (acc[at] + pair[j].astype(f32)).astype(bf16)
        return carry

    lax.fori_loop(0, half, add_pair, 0)
    precv[chip] = psend[me]
    send_chips(3, lambda to: psend.at[2 * to + core], precv, chip)
    lax.fori_loop(1, blocks, center_grads, 0)

    wait_all(rsems, 3, precv, half - 1)
    grad_dir = jnp.sum(precv[...].astype(f32), axis=0)
    own = esend[...].astype(f32)
    inv_emb = inverse_norm(own)
    emb_dir = own * inv_emb
    along = jnp.sum(grad_dir * emb_dir, axis=1, keepdims=True)
    grad_emb = ((grad_dir - emb_dir * along) * inv_emb).astype(bf16)
    gsend[...] = grad_emb
    grecv[me] = grad_emb
    send_chips(4, lambda to: gsend, grecv, me)

    wait_all(rsems, 1, frecv, n - 1)
    for k in range(max(blocks - 2, 0), blocks):
        out_copy(k, k % 2).wait()
    wait_all(rsems, 4, grecv, half - 1)
    send_partner(7, lambda j: grecv.at[2 * j + core], lambda j: grecv.at[2 * j + core])
    wait_all(rsems, 7, grecv, half)
    fc_out[...] = lax.dot_general(
        frecv[...].reshape(batch, part), grecv[...].reshape(batch, width),
        (((0,), (0,)), ((), ())), preferred_element_type=f32,
    )
    wait_all(ssems, 0, emb, half - 1)
    wait_all(ssems, 1, frecv, n - 1)
    wait_all(ssems, 2, srecv, n - 1)
    wait_all(ssems, 3, precv, half - 1)
    wait_all(ssems, 4, grecv, half - 1)
    wait_all(ssems, 6, pair, half)
    wait_all(ssems, 7, grecv, half)


def on_device(features, fc_weight, centers, labels):
    n = lax.axis_size("cls")
    tok, feats = features.shape
    classes, width = centers.shape
    batch = labels.shape[0]
    rows = min(512, 262144 // batch)
    slots = 4 if batch <= 1024 else 2
    chunk = 128 * largest_divisor(feats // 128, 14)
    part = feats // n
    vmem = pl.BlockSpec(memory_space=pltpu.VMEM)
    hbm = pl.BlockSpec(memory_space=pl.ANY)
    loss_row, grad_centers, grad_fc = pl.pallas_call(
        functools.partial(kernel, n, rows, slots),
        out_shape=(
            jax.ShapeDtypeStruct((1, batch), f32),
            jax.ShapeDtypeStruct((classes, width), bf16),
            jax.ShapeDtypeStruct((part, width), f32),
        ),
        in_specs=[vmem, hbm, hbm, vmem],
        out_specs=(vmem, hbm, vmem),
        scratch_shapes=[
            pltpu.VMEM((slots, chunk, width), bf16),
            pltpu.VMEM((classes, width), bf16),
            pltpu.VMEM((classes, width), bf16),
            pltpu.VMEM((classes, 1), f32),
            pltpu.VMEM((classes, batch), f32),
            pltpu.VMEM((batch, width), f32),
            pltpu.VMEM((tok, width), bf16),
            pltpu.VMEM((n, tok, width), bf16),
            pltpu.VMEM((n, tok, part), bf16),
            pltpu.VMEM((n, tok, part), bf16),
            pltpu.VMEM((2, batch), f32),
            pltpu.VMEM((n, 2, batch), f32),
            pltpu.VMEM((n, tok, width), bf16),
            pltpu.VMEM((n // 2, tok, width), bf16),
            pltpu.VMEM((n // 2, tok, width), bf16),
            pltpu.VMEM((tok, width), bf16),
            pltpu.VMEM((n, tok, width), bf16),
            pltpu.VMEM((2, rows, width), bf16),
            pltpu.SemaphoreType.DMA((slots,)),
            pltpu.SemaphoreType.DMA,
            pltpu.SemaphoreType.DMA((2,)),
            pltpu.SemaphoreType.DMA((8,)),
            pltpu.SemaphoreType.DMA((8,)),
        ],
        compiler_params=pltpu.CompilerParams(
            collective_id=0, has_side_effects=True, vmem_limit_bytes=67043328
        ),
    )(features, fc_weight, centers, labels[None])
    loss = lax.dynamic_slice_in_dim(loss_row[0], lax.axis_index("cls") * tok, tok)
    return (loss, grad_centers, grad_fc)


def solution(mesh):
    placed = (P("cls", None), P(), P("cls", None), P())
    return jax.shard_map(
        on_device,
        mesh=mesh,
        in_specs=placed,
        out_specs=(P("cls"), P("cls", None), P("cls", None)),
        check_vma=False,
    )
```
